32 devices in a mesh: pb: 4 (over y, core), pa: 8 (over z, x).
Axes of the slice: x: 2, y: 2, z: 4, core: 2. Of those that a mesh axis runs over, the one named last changes fastest.
Arguments:
- query_hidden: bfloat16 [32, 32, 2048], P('pb', 'pa'), may hold values from -32 to 32
- page_hidden: bfloat16 [8, 1024, 2048], P('pa', 'pb'), may hold values from -4.2 to 4.2
- projection: bfloat16 [2048, 128], replicated, may hold values from -0.125 to 0.125
- clicks: int32 [32, 8, 2], P('pb'), may hold values from 0 to 7, as said below
- bins: int32 [32, 8], P('pb'), may hold values from 0 to 7
Outputs:
- query_grad: bfloat16 [32, 32, 2048], P('pb', 'pa')
- page_grad: bfloat16 [8, 1024, 2048], P('pa', 'pb')
- weight_grad: float32 [2048, 128], P(('pb', 'pa'))
The draws below stay inside these ranges and needn't reach their ends.
Inputs may be any that keep to these rules, and one draw needn't show every extreme that they name: `clicks`: the two pages of a pair always differ.
All inputs are finite; a program needn't handle non-finite values.
Results may differ from the reference program's by a relative error of at most 0.019.
Values may be sent and summed in bfloat16 or wider, within the bound.
A program may use at most 64 MiB of HBM per device.

```python
import jax
import jax.numpy as jnp
from jax import lax

D = 2048
E = 128
NPATCH = 1024
LQ = 32
PAIRS = 8
BINS = 8
NQ = 32
NP = 8


def query_base(key):
    return jax.random.truncated_normal(jax.random.fold_in(key, 1), -4.0, 4.0, (NQ, LQ, D), jnp.float32)


def draw_query_hidden(key, part):
    values = query_base(key)
    return values.astype(jnp.bfloat16)


def draw_page_hidden(key, part):
    values = jax.random.truncated_normal(jax.random.fold_in(key, 2), -4.0, 4.0, (NP, NPATCH, D), jnp.float32)
    return values.astype(jnp.bfloat16)


def draw_clicks(key, part):
    positive = jax.random.randint(jax.random.fold_in(key, 3), (NQ, PAIRS), 0, NP)
    offset = jax.random.randint(jax.random.fold_in(key, 4), (NQ, PAIRS), 1, NP)
    negative = (positive + offset) % NP
    return jnp.stack([positive, negative], axis=2).astype(jnp.int32)


def place_ends(values, own_key, low, high):
    index_at = [jax.random.randint(jax.random.fold_in(own_key, axis), (), 0, length) for axis, length in enumerate(values.shape)]
    main_axis = values.shape.index(max(values.shape))
    neighbour = index_at[:main_axis] + [(index_at[main_axis] + 1) % values.shape[main_axis]] + index_at[main_axis + 1:]
    return values.at[tuple(index_at)].set(low).at[tuple(neighbour)].set(high)


def noise(rng, extent, spread, reach, kind=jnp.bfloat16):
    drawn = spread * jax.random.normal(rng, extent, jnp.float32)
    return jnp.clip(drawn, min=-reach, max=reach).astype(kind)


def setup_inputs(seed: int = 0) -> dict:
    splits = jax.random.split(jax.random.key(seed), 6)
    return {
        "query_hidden": draw_query_hidden(jax.random.fold_in(splits[5], 71), 0),
        "page_hidden": draw_page_hidden(jax.random.fold_in(splits[5], 71), 0),
        "projection": noise(splits[2], (D, E), D ** -0.5, 0.125),
        "clicks": draw_clicks(jax.random.fold_in(splits[5], 71), 0),
        "bins": place_ends(jax.random.randint(splits[4], (NQ, PAIRS), 0, BINS), jax.random.fold_in(splits[4], 1), 0, BINS - 1).astype(jnp.int32),
    }


sharpness = 0.25

def reference(query_hidden, page_hidden, projection, clicks, bins):
    hidden_width = query_hidden.shape[2]
    query_embed = jnp.dot(query_hidden.reshape(-1, hidden_width), projection, preferred_element_type=jnp.float32).astype(jnp.bfloat16)
    page_embed = jnp.dot(page_hidden.reshape(-1, hidden_width), projection, preferred_element_type=jnp.float32).astype(jnp.bfloat16).reshape(NP, NPATCH, E)

    def page_norm(page_block):
        logit_block = sharpness * jnp.dot(query_embed, page_block.T, preferred_element_type=jnp.float32)
        return jax.nn.logsumexp(logit_block, axis=1)
    log_norm = lax.map(page_norm, page_embed)
    query_score = log_norm.T.reshape(NQ, LQ, NP).sum(axis=1)
    page_ids = jnp.arange(NP, dtype=jnp.int32)
    hit_pos = (clicks[:, :, 0][:, :, None] == page_ids).astype(jnp.float32)
    hit_neg = (clicks[:, :, 1][:, :, None] == page_ids).astype(jnp.float32)
    pair_gap = lax.optimization_barrier(jnp.sum(hit_pos * query_score[:, None, :], axis=2)) - lax.optimization_barrier(jnp.sum(hit_neg * query_score[:, None, :], axis=2))
    pair_weight = jnp.sqrt(bins.astype(jnp.float32) + 1.0)
    pair_coeff = -pair_weight * jax.nn.sigmoid(-pair_gap)
    score_grad = lax.optimization_barrier(jnp.sum(pair_coeff[:, :, None] * (hit_pos - hit_neg), axis=1))
    grad_rows = jnp.repeat(score_grad, LQ, axis=0)

    def page_back(token_acc, inputs):
        page_block, norm_col, grad_col = inputs
        logit_block = sharpness * jnp.dot(query_embed, page_block.T, preferred_element_type=jnp.float32)
        soft_grad = (grad_col[:, None] * jnp.exp(logit_block - norm_col[:, None])).astype(jnp.bfloat16)
        token_acc = token_acc + jnp.dot(soft_grad, page_block, preferred_element_type=jnp.float32)
        patch_part = jnp.dot(soft_grad.T, query_embed, preferred_element_type=jnp.float32)
        return (token_acc, patch_part)
    token_acc, patch_acc = lax.scan(page_back, jnp.zeros((NQ * LQ, E), jnp.float32), (page_embed, log_norm, grad_rows.T))
    token_low = (sharpness * token_acc).astype(jnp.bfloat16)
    patch_low = (sharpness * patch_acc).astype(jnp.bfloat16).reshape(-1, E)
    query_grad = jnp.dot(token_low, projection.T, preferred_element_type=jnp.float32).astype(jnp.bfloat16).reshape(query_hidden.shape)
    page_grad = jnp.dot(patch_low, projection.T, preferred_element_type=jnp.float32).astype(jnp.bfloat16).reshape(page_hidden.shape)
    weight_grad = jnp.dot(query_hidden.reshape(-1, hidden_width).T, token_low, preferred_element_type=jnp.float32)
    weight_grad = weight_grad + jnp.dot(page_hidden.reshape(-1, hidden_width).T, patch_low, preferred_element_type=jnp.float32)
    return (query_grad, page_grad, weight_grad)
```

```python
import functools

import jax
import jax.numpy as jnp
from jax import lax
from jax.experimental import pallas as pl
from jax.experimental.pallas import tpu as pltpu
from jax.sharding import PartitionSpec as P

sharpness = 0.25
MESH = pl.DeviceIdType.MESH
BF = jnp.bfloat16
F32 = jnp.float32


def dot(x, y, dims):
    return lax.dot_general(x, y, (dims, ((), ())), preferred_element_type=F32)


def kernel(
    PB, PA, qh_ref, ph_ref, proj_ref, pos_ref, neg_ref, weight_ref, mask_ref,
    tlow_ref, plow_ref, w_ref,
    qe, pe, ebuf, sc, gsend, grecv, tsend, trecv, w1send, w1recv, wown, w2send, w2recv,
    qs, qr, ps, pr, ss, sr, gs, gr, ts, tr, us, ur, vs, vr,
):
    b = lax.axis_index("pb")
    a = lax.axis_index("pa")
    rows = qh_ref.shape[0]
    E = proj_ref.shape[1]
    tokens = PA * rows

    def remote(src, dst, send, recv, to_b, to_a):
        return pltpu.make_async_remote_copy(
            src_ref=src, dst_ref=dst, send_sem=send, recv_sem=recv,
            device_id=(to_b, to_a), device_id_type=MESH,
        )

    barrier = pltpu.get_barrier_semaphore()

    def greet(k, carry):
        other = lax.rem(b * PA + a + k, PB * PA)
        pl.semaphore_signal(
            barrier, inc=1, device_id=(other // PA, lax.rem(other, PA)), device_id_type=MESH
        )
        return carry

    lax.fori_loop(1, PB * PA, greet, 0)

    qe[a] = dot(qh_ref[...], proj_ref[...], ((1,), (0,))).astype(BF)
    pe[b] = dot(ph_ref[...], proj_ref[...], ((1,), (0,))).astype(BF)
    pl.semaphore_wait(barrier, PB * PA - 1)

    copies = []
    page_in = {}
    for o in range(1, PB):
        c = remote(pe.at[b], pe.at[b], ps.at[o - 1], pr.at[o - 1], lax.rem(b + o, PB), a)
        c.start()
        page_in[o] = c
    query_in = []
    for o in range(1, PA):
        c = remote(qe.at[a], qe.at[a], qs.at[o - 1], qr.at[o - 1], b, lax.rem(a + o, PA))
        c.start()
        query_in.append(c)
    for c in query_in:
        c.wait_recv()

    tok = qe[...].reshape(tokens, E)
    maxes, sums = [], []
    for o in range(PB):
        j = lax.rem(b + PB - o, PB)
        if o:
            page_in[o].wait_recv()
        block = sharpness * dot(pe[j], tok, ((1,), (1,)))
        top = jnp.max(block, axis=0, keepdims=True)
        e = jnp.exp(block - top)
        ebuf[o] = e
        maxes.append(top)
        sums.append(jnp.sum(e, axis=0, keepdims=True))
    top = functools.reduce(jnp.maximum, maxes)
    shrink = [jnp.exp(m - top) for m in maxes]
    total = functools.reduce(jnp.add, [s * f for s, f in zip(sums, shrink)])
    log_norm = top + jnp.log(total)
    mask = mask_ref[...]
    score = jnp.sum(mask * log_norm, axis=1, keepdims=True)
    sc[a] = jnp.broadcast_to(score, sc.shape[1:])
    score_in = []
    for o in range(1, PA):
        c = remote(sc.at[a], sc.at[a], ss.at[o - 1], sr.at[o - 1], b, lax.rem(a + o, PA))
        c.start()
        score_in.append(c)
    for c in score_in:
        c.wait_recv()

    pos = pos_ref[...]
    neg = neg_ref[...]
    at_pos = jnp.zeros(pos.shape, F32)
    at_neg = jnp.zeros(pos.shape, F32)
    for p in range(PA):
        at_pos = at_pos + jnp.where(pos == p, sc[p], 0.0)
        at_neg = at_neg + jnp.where(neg == p, sc[p], 0.0)
    coeff = -weight_ref[...] * jax.nn.sigmoid(at_neg - at_pos)
    hits = (pos == a).astype(F32) - (neg == a).astype(F32)
    grad = jnp.sum(coeff * hits, axis=1, keepdims=True)
    grad_row = jnp.sum(mask * grad, axis=0, keepdims=True) / total

    token_acc = None
    patch_in = []
    for o in list(range(1, PB)) + [0]:
        j = lax.rem(b + PB - o, PB)
        soft = (ebuf[o] * (grad_row * shrink[o])).astype(BF)
        patch_part = dot(soft, tok, ((1,), (0,)))
        if o:
            gsend[o - 1] = patch_part.astype(BF)
            c = remote(gsend.at[o - 1], grecv.at[o - 1], gs.at[o - 1], gr.at[o - 1], j, a)
            c.start()
            patch_in.append(c)
        else:
            patch_acc = patch_part
        part = dot(soft, pe[j], ((0,), (0,)))
        token_acc = part if token_acc is None else token_acc + part
    for k in range(PA):
        tsend[k] = token_acc[k * rows:(k + 1) * rows].astype(BF)
    token_in = []
    for o in range(1, PA):
        to = lax.rem(a + o, PA)
        c = remote(tsend.at[to], trecv.at[o - 1], ts.at[o - 1], tr.at[o - 1], b, to)
        c.start()
        token_in.append(c)
    token_own = tsend[a].astype(F32)
    for o, c in enumerate(patch_in):
        c.wait_recv()
        patch_acc = patch_acc + grecv[o].astype(F32)
    patch_low = (sharpness * patch_acc).astype(BF)
    plow_ref[...] = patch_low
    for o, c in enumerate(token_in):
        c.wait_recv()
        token_own = token_own + trecv[o].astype(F32)
    token_low = (sharpness * token_own).astype(BF)
    tlow_ref[...] = token_low

    half = PB // 2
    parity = lax.rem(b, 2)
    partner = b + 1 - 2 * parity
    span = w1send.shape[1]
    chunk = w_ref.shape[0]

    def weight_block(index):
        cols = pl.ds(pl.multiple_of(index * span, 128), span)
        return dot(ph_ref[:, cols], patch_low, ((0,), (0,))) + dot(
            qh_ref[:, cols], token_low, ((0,), (0,))
        )

    pair_in = []
    for m in range(half):
        w1send[m] = weight_block(2 * m + 1 - parity).astype(BF)
        c = remote(w1send.at[m], w1recv.at[m], us.at[m], ur.at[m], partner, a)
        c.start()
        pair_in.append(c)
    for m in range(half):
        wown[m] = weight_block(2 * m + parity)
    for m in range(half):
        pair_in[m].wait_recv()
        both = (wown[m] + w1recv[m].astype(F32)).astype(BF)
        for k in range(PA):
            w2send[m * PA + k] = both[k * chunk:(k + 1) * chunk]
    count = half * PA
    mine = (b // 2) * PA + a
    last_in = []
    for o in range(1, count):
        to = lax.rem(mine + o, count)
        c = remote(
            w2send.at[to], w2recv.at[o - 1], vs.at[o - 1], vr.at[o - 1],
            2 * (to // PA) + parity, lax.rem(to, PA),
        )
        c.start()
        last_in.append(c)
    weight = w2send[mine].astype(F32)
    for o, c in enumerate(last_in):
        c.wait_recv()
        weight = weight + w2recv[o].astype(F32)
    w_ref[...] = weight
    for c in list(page_in.values()) + query_in + score_in + patch_in + token_in + pair_in + last_in:
        c.wait_send()


def shards(PB, PA, query_hidden, page_hidden, projection, clicks, bins):
    queries, token_local, hidden = query_hidden.shape
    page_count, patches, _ = page_hidden.shape
    assert page_count == 1 and PB % 2 == 0
    pairs = clicks.shape[1]
    E = projection.shape[1]
    rows = queries * token_local
    tokens = rows * PA
    chunk = hidden // (PB * PA)
    half = PB // 2
    count = half * PA
    lanes = -(-pairs // 128) * 128
    pad = ((0, 0), (0, lanes - pairs))
    pos = jnp.pad(clicks[:, :, 0], pad, constant_values=-1)
    neg = jnp.pad(clicks[:, :, 1], pad, constant_values=-1)
    weight = jnp.pad(jnp.sqrt(bins.astype(F32) + 1.0), pad)
    mask = (
        (jnp.arange(tokens)[None, :] % rows) // token_local == jnp.arange(queries)[:, None]
    ).astype(F32)
    qh = query_hidden.reshape(rows, hidden)
    ph = page_hidden.reshape(patches, hidden)
    vmem = pl.BlockSpec(memory_space=pltpu.VMEM)
    dma = lambda n: pltpu.SemaphoreType.DMA((n,))
    token_low, patch_low, weight_grad = pl.pallas_call(
        functools.partial(kernel, PB, PA),
        out_shape=(
            jax.ShapeDtypeStruct((rows, E), BF),
            jax.ShapeDtypeStruct((patches, E), BF),
            jax.ShapeDtypeStruct((chunk, E), F32),
        ),
        in_specs=[vmem] * 7,
        out_specs=(vmem,) * 3,
        scratch_shapes=[
            pltpu.VMEM((PA, rows, E), BF),
            pltpu.VMEM((PB, patches, E), BF),
            pltpu.VMEM((PB, patches, tokens), F32),
            pltpu.VMEM((PA, queries, lanes), F32),
            pltpu.VMEM((PB - 1, patches, E), BF),
            pltpu.VMEM((PB - 1, patches, E), BF),
            pltpu.VMEM((PA, rows, E), BF),
            pltpu.VMEM((PA - 1, rows, E), BF),
            pltpu.VMEM((half, PA * chunk, E), BF),
            pltpu.VMEM((half, PA * chunk, E), BF),
            pltpu.VMEM((half, PA * chunk, E), F32),
            pltpu.VMEM((count, chunk, E), BF),
            pltpu.VMEM((count - 1, chunk, E), BF),
            dma(PA - 1), dma(PA - 1), dma(PB - 1), dma(PB - 1), dma(PA - 1), dma(PA - 1),
            dma(PB - 1), dma(PB - 1), dma(PA - 1), dma(PA - 1), dma(half), dma(half),
            dma(count - 1), dma(count - 1),
        ],
        compiler_params=pltpu.CompilerParams(
            collective_id=0, has_side_effects=True, vmem_limit_bytes=48 * 1024 * 1024
        ),
        name="fused",
    )(qh, ph, projection, pos, neg, weight, mask)
    query_grad = dot(token_low, projection, ((1,), (1,))).astype(BF).reshape(query_hidden.shape)
    page_grad = dot(patch_low, projection, ((1,), (1,))).astype(BF).reshape(page_hidden.shape)
    return query_grad, page_grad, weight_grad


def solution(mesh):
    return jax.shard_map(
        functools.partial(shards, mesh.shape["pb"], mesh.shape["pa"]),
        mesh=mesh,
        in_specs=(
            P("pb", "pa", None),
            P("pa", "pb", None),
            P(),
            P("pb", None, None),
            P("pb", None),
        ),
        out_specs=(P("pb", "pa", None), P("pa", "pb", None), P(("pb", "pa"), None)),
        check_vma=False,
    )
```

```python
import functools

import jax
import jax.numpy as jnp
from jax import lax
from jax.experimental import pallas as pl
from jax.experimental.pallas import tpu as pltpu
from jax.sharding import PartitionSpec as P

sharpness = 0.25
MESH = pl.DeviceIdType.MESH
BF = jnp.bfloat16
F32 = jnp.float32


def dot(x, y, dims):
    return lax.dot_general(x, y, (dims, ((), ())), preferred_element_type=F32)


def kernel(
    PB, PA, qh_hbm, ph_hbm, proj_hbm, clicks_hbm, bins_hbm,
    qg_ref, pg_ref, w_ref,
    clicks_ref, bins_ref, qraw, qh, ph, pht, proj, qe, pe, ebuf, pbuf, sc, gsend, grecv, tsend, trecv,
    wq, w1send, w1recv, w2send, w2recv,
    ls, qs, qr, ps, pr, ss, sr, gs, gr, ts, tr, us, ur, vs, vr,
):
    b = lax.axis_index("pb")
    a = lax.axis_index("pa")
    queries, token_local, hidden = qh_hbm.shape
    rows = queries * token_local
    E = proj.shape[1]
    tokens = PA * rows
    half = PB // 2
    parity = lax.rem(b, 2)
    level = b // 2

    def remote(src, dst, send, recv, to_b, to_a):
        return pltpu.make_async_remote_copy(
            src_ref=src, dst_ref=dst, send_sem=send, recv_sem=recv,
            device_id=(to_b, to_a), device_id_type=MESH,
        )

    loads = [
        pltpu.make_async_copy(qh_hbm, qraw, ls.at[0]),
        pltpu.make_async_copy(proj_hbm, proj, ls.at[1]),
        pltpu.make_async_copy(ph_hbm, ph, ls.at[2]),
        pltpu.make_async_copy(clicks_hbm, clicks_ref, ls.at[3]),
        pltpu.make_async_copy(bins_hbm, bins_ref, ls.at[4]),
    ]
    for c in loads:
        c.start()
    barrier = pltpu.get_barrier_semaphore()

    def greet(k, carry):
        other = lax.rem(b * PA + a + k, PB * PA)
        pl.semaphore_signal(
            barrier, inc=1, device_id=(other // PA, lax.rem(other, PA)), device_id_type=MESH
        )
        return carry

    lax.fori_loop(1, PB * PA, greet, 0)

    def group(k):
        return 2 * lax.rem(level + half - k // 2, half) + lax.rem(parity + k % 2, 2)

    def source(k):
        return 2 * lax.rem(level + k // 2, half) + lax.rem(parity + k % 2, 2)

    loads[0].wait()
    for q in range(queries):
        qh[q * token_local:(q + 1) * token_local] = qraw[q].astype(F32)
    loads[1].wait()
    qrows = qh[...].astype(BF)
    qe[a] = dot(qrows, proj[...], ((1,), (0,))).astype(BF)
    loads[2].wait()
    pe[b] = dot(ph[...], proj[...], ((1,), (0,))).astype(BF)
    pl.semaphore_wait(barrier, PB * PA - 1)

    query_in = []
    for o in range(1, PA):
        c = remote(qe.at[a], qe.at[a], qs.at[o - 1], qr.at[o - 1], b, lax.rem(a + o, PA))
        c.start()
        query_in.append(c)
    page_in = {}
    for k in range(PB - 1, 0, -1):
        c = remote(pe.at[b], pe.at[b], ps.at[k - 1], pr.at[k - 1], group(k), a)
        c.start()
        page_in[k] = c

    step = min(256, hidden)
    for s in range(0, hidden, step):
        pht[s:s + step] = ph[:, s:s + step].T

    for c in query_in:
        c.wait_recv()
    tok = qe[...].reshape(tokens, E)
    row = lax.broadcasted_iota(jnp.int32, (queries, tokens), 0) * token_local
    col = lax.broadcasted_iota(jnp.int32, (queries, tokens), 1)
    mask = jnp.zeros((queries, tokens), F32)
    for k in range(PA):
        low = row + k * rows
        mask = jnp.where((col >= low) & (col < low + token_local), 1.0, mask)
    maxes, sums = [], []
    for k in range(PB):
        if k:
            page_in[k].wait_recv()
        block = sharpness * dot(pe[source(k)], tok, ((1,), (1,)))
        top = jnp.max(block, axis=0, keepdims=True)
        e = jnp.exp(block - top)
        ebuf[k] = e
        maxes.append(top)
        sums.append(jnp.sum(e, axis=0, keepdims=True))
    top = functools.reduce(jnp.maximum, maxes)
    shrink = [jnp.exp(m - top) for m in maxes]
    total = functools.reduce(jnp.add, [s * f for s, f in zip(sums, shrink)])
    log_norm = top + jnp.log(total)
    score = jnp.sum(mask * log_norm, axis=1, keepdims=True)
    sc[a] = jnp.broadcast_to(score, sc.shape[1:])
    score_in = []
    for o in range(1, PA):
        c = remote(sc.at[a], sc.at[a], ss.at[o - 1], sr.at[o - 1], b, lax.rem(a + o, PA))
        c.start()
        score_in.append(c)

    unit = None
    for k in range(PB):
        soft = (ebuf[k] * (shrink[k] / total)).astype(BF)
        pbuf[k] = soft
        part = dot(soft, pe[source(k)], ((0,), (0,)))
        unit = part if unit is None else unit + part
    for k in range(PA):
        tsend[k] = unit[k * rows:(k + 1) * rows].astype(BF)
    token_in = []
    for o in range(1, PA):
        to = lax.rem(a + o, PA)
        c = remote(tsend.at[to], trecv.at[a], ts.at[o - 1], tr.at[o - 1], b, to)
        c.start()
        token_in.append(c)
    trecv[a] = tsend[a]

    loads[3].wait()
    loads[4].wait()
    pos = clicks_ref[:, 0, :]
    neg = clicks_ref[:, 1, :]
    pairs = pos.shape[1]
    weight = jnp.sqrt(bins_ref[...].astype(F32) + 1.0)
    for c in score_in:
        c.wait_recv()
    at_pos = jnp.zeros(pos.shape, F32)
    at_neg = jnp.zeros(pos.shape, F32)
    for p in range(PA):
        at_pos = at_pos + jnp.where(pos == p, sc[p][:, :pairs], 0.0)
        at_neg = at_neg + jnp.where(neg == p, sc[p][:, :pairs], 0.0)
    coeff = -weight * jax.nn.sigmoid(at_neg - at_pos)
    row = lax.broadcasted_iota(jnp.int32, (rows, queries), 0)
    col = lax.broadcasted_iota(jnp.int32, (rows, queries), 1) * token_local
    own = jnp.where((row >= col) & (row < col + token_local), 1.0, 0.0)

    def spread(page):
        hits = (pos == page).astype(F32) - (neg == page).astype(F32)
        grad = jnp.sum(coeff * hits, axis=1, keepdims=True)
        return sum(own[:, q:q + 1] * grad[q:q + 1] for q in range(queries))

    scaled = (qe[...].astype(F32) * spread(a)[None]).astype(BF).reshape(tokens, E)
    patch_in = []
    for k in range(PB - 1, -1, -1):
        patch_part = dot(pbuf[k], scaled, ((1,), (0,)))
        if k:
            gsend[k - 1] = patch_part.astype(BF)
            c = remote(
                gsend.at[k - 1], grecv.at[k - 1], gs.at[k - 1], gr.at[k - 1],
                source(k), a,
            )
            c.start()
            patch_in.append((k, c))
        else:
            patch_acc = patch_part

    for c in token_in:
        c.wait_recv()
    token_own = None
    for p in range(PA):
        part = trecv[p].astype(F32) * spread(p)
        token_own = part if token_own is None else token_own + part
    token_low = (sharpness * token_own).astype(BF)
    wq[...] = dot(qrows, token_low, ((0,), (0,)))
    qgrad = dot(token_low, proj[...], ((1,), (1,)))
    for q in range(queries):
        qg_ref[q] = qgrad[q * token_local:(q + 1) * token_local].astype(BF)

    for k, c in reversed(patch_in):
        c.wait_recv()
        patch_acc = patch_acc + grecv[k - 1].astype(F32)
    patch_low = (sharpness * patch_acc).astype(BF)

    partner = b + 1 - 2 * parity
    span = w1send.shape[1]
    chunk = w_ref.shape[0]
    def weight_block(index):
        base = pl.multiple_of(index * span, 8)
        return wq[pl.ds(base, span)] + dot(pht[pl.ds(base, span)], patch_low, ((1,), (0,)))

    pair_in = {}
    for m in range(half - 1, -1, -1):
        w1send[m] = weight_block(2 * lax.rem(level + m, half) + 1 - parity).astype(BF)
        c = remote(w1send.at[m], w1recv.at[m], us.at[m], ur.at[m], partner, a)
        c.start()
        pair_in[m] = c
    last_in = []
    weight_own = None
    for m in range(half - 1, -1, -1):
        to_level = lax.rem(level + m, half)
        mine = weight_block(2 * to_level + parity)
        pair_in[m].wait_recv()
        both = (mine + w1recv[m].astype(F32)).astype(BF)
        for k in range(PA):
            w2send[m * PA + k] = both[k * chunk:(k + 1) * chunk]
        for o in range(PA - 1, -1, -1):
            slot = m * PA + o
            if slot:
                to = lax.rem(a + o, PA)
                c = remote(
                    w2send.at[m * PA + to], w2recv.at[slot - 1], vs.at[slot - 1],
                    vr.at[slot - 1], 2 * to_level + parity, to,
                )
                c.start()
                last_in.append((slot, c))
    pg_ref[...] = dot(patch_low, proj[...], ((1,), (1,))).astype(BF)
    weight_sum = w2send[a].astype(F32)
    for slot, c in last_in:
        c.wait_recv()
        weight_sum = weight_sum + w2recv[slot - 1].astype(F32)
    w_ref[...] = weight_sum
    last_in = [c for _, c in last_in]
    pair_in = list(pair_in.values())
    for c in list(page_in.values()) + query_in + score_in + [c for _, c in patch_in] + token_in + pair_in + last_in:
        c.wait_send()


def writer(qg, pg, w, qg_out, pg_out, w_out, sems):
    copies = [
        pltpu.make_async_copy(pg, pg_out, sems.at[0]),
        pltpu.make_async_copy(qg, qg_out, sems.at[1]),
        pltpu.make_async_copy(w, w_out, sems.at[2]),
    ]
    for c in copies:
        c.start()
    for c in copies:
        c.wait()


def shards(PB, PA, query_hidden, page_hidden, projection, clicks, bins):
    queries, token_local, hidden = query_hidden.shape
    page_count, patches, _ = page_hidden.shape
    assert page_count == 1 and PB % 2 == 0
    E = projection.shape[1]
    rows = queries * token_local
    tokens = rows * PA
    chunk = hidden // (PB * PA)
    half = PB // 2
    count = half * PA
    ph = page_hidden.reshape(patches, hidden)
    vmem = pl.BlockSpec(memory_space=pltpu.VMEM)
    hbm = pl.BlockSpec(memory_space=pltpu.HBM)
    dma = lambda n: pltpu.SemaphoreType.DMA((n,))
    outs = (
        jax.ShapeDtypeStruct(query_hidden.shape, BF),
        jax.ShapeDtypeStruct((patches, hidden), BF),
        jax.ShapeDtypeStruct((chunk, E), F32),
    )
    results = pl.pallas_call(
        functools.partial(kernel, PB, PA),
        out_shape=tuple(pltpu.VMEM(o.shape, o.dtype) for o in outs),
        in_specs=[hbm] * 5,
        out_specs=(vmem,) * 3,
        scratch_shapes=[
            pltpu.VMEM((queries, 2, clicks.shape[1]), jnp.int32),
            pltpu.VMEM(bins.shape, jnp.int32),
            pltpu.VMEM(query_hidden.shape, BF),
            pltpu.VMEM((rows, hidden), F32),
            pltpu.VMEM((patches, hidden), BF),
            pltpu.VMEM((hidden, patches), BF),
            pltpu.VMEM((hidden, E), BF),
            pltpu.VMEM((PA, rows, E), BF),
            pltpu.VMEM((PB, patches, E), BF),
            pltpu.VMEM((PB, patches, tokens), F32),
            pltpu.VMEM((PB, patches, tokens), BF),
            pltpu.VMEM((PA, queries, 128), F32),
            pltpu.VMEM((PB - 1, patches, E), BF),
            pltpu.VMEM((PB - 1, patches, E), BF),
            pltpu.VMEM((PA, rows, E), BF),
            pltpu.VMEM((PA, rows, E), BF),
            pltpu.VMEM((hidden, E), F32),
            pltpu.VMEM((half, PA * chunk, E), BF),
            pltpu.VMEM((half, PA * chunk, E), BF),
            pltpu.VMEM((count, chunk, E), BF),
            pltpu.VMEM((count - 1, chunk, E), BF),
            dma(5), dma(PA - 1), dma(PA - 1), dma(PB - 1), dma(PB - 1), dma(PA - 1), dma(PA - 1),
            dma(PB - 1), dma(PB - 1), dma(PA - 1), dma(PA - 1), dma(half), dma(half),
            dma(count - 1), dma(count - 1),
        ],
        compiler_params=pltpu.CompilerParams(
            collective_id=0, has_side_effects=True, vmem_limit_bytes=65536000
        ),
        name="fused",
    )(query_hidden, ph, projection, jnp.transpose(clicks, (0, 2, 1)), bins)
    query_grad, page_grad, weight_grad = pl.pallas_call(
        writer,
        out_shape=outs,
        in_specs=[vmem] * 3,
        out_specs=(hbm,) * 3,
        scratch_shapes=[dma(3)],
        compiler_params=pltpu.CompilerParams(vmem_limit_bytes=4 * 1024 * 1024),
        name="writer",
    )(*results)
    return query_grad, page_grad.reshape(page_hidden.shape), weight_grad


def solution(mesh):
    return jax.shard_map(
        functools.partial(shards, mesh.shape["pb"], mesh.shape["pa"]),
        mesh=mesh,
        in_specs=(
            P("pb", "pa", None),
            P("pa", "pb", None),
            P(),
            P("pb", None, None),
            P("pb", None),
        ),
        out_specs=(P("pb", "pa", None), P("pa", "pb", None), P(("pb", "pa"), None)),
        check_vma=False,
    )
```

```python
import functools

import jax
import jax.numpy as jnp
from jax import lax
from jax.experimental import pallas as pl
from jax.experimental.pallas import tpu as pltpu
from jax.sharding import PartitionSpec as P

sharpness = 0.25
MESH = pl.DeviceIdType.MESH
BF = jnp.bfloat16
F32 = jnp.float32


def dot(x, y, dims):
    return lax.dot_general(x, y, (dims, ((), ())), preferred_element_type=F32)


def kernel(
    PB, PA, qh_hbm, ph_hbm, proj_hbm, clicks_hbm, bins_hbm,
    qg_ref, pg_ref, w_ref,
    clicks_ref, bins_ref, qraw, qh, ph, pht, proj, qe, pe, ebuf, pbuf, sc, gsend, grecv, tsend, trecv,
    wq, w1send, w1recv, w2send, w2recv,
    ls, qs, qr, ps, pr, ss, sr, gs, gr, ts, tr, us, ur, vs, vr,
):
    b = lax.axis_index("pb")
    a = lax.axis_index("pa")
    queries, token_local, hidden = qh_hbm.shape
    rows = queries * token_local
    E = proj.shape[1]
    tokens = PA * rows
    half = PB // 2
    parity = lax.rem(b, 2)
    level = b // 2

    def remote(src, dst, send, recv, to_b, to_a):
        return pltpu.make_async_remote_copy(
            src_ref=src, dst_ref=dst, send_sem=send, recv_sem=recv,
            device_id=(to_b, to_a), device_id_type=MESH,
        )

    loads = [
        pltpu.make_async_copy(qh_hbm, qraw, ls.at[0]),
        pltpu.make_async_copy(proj_hbm, proj, ls.at[1]),
        pltpu.make_async_copy(ph_hbm, ph, ls.at[2]),
        pltpu.make_async_copy(clicks_hbm, clicks_ref, ls.at[3]),
        pltpu.make_async_copy(bins_hbm, bins_ref, ls.at[4]),
    ]
    for c in loads:
        c.start()
    barrier = pltpu.get_barrier_semaphore()

    for o in range(1, PA):
        pl.semaphore_signal(
            barrier, inc=1, device_id=(b, lax.rem(a + o, PA)), device_id_type=MESH
        )
    for o in range(1, PB):
        pl.semaphore_signal(
            barrier, inc=1, device_id=(lax.rem(b + o, PB), a), device_id_type=MESH
        )

    def group(k):
        return 2 * lax.rem(level + half - k // 2, half) + lax.rem(parity + k % 2, 2)

    def source(k):
        return 2 * lax.rem(level + k // 2, half) + lax.rem(parity + k % 2, 2)

    loads[0].wait()
    for q in range(queries):
        qh[q * token_local:(q + 1) * token_local] = qraw[q].astype(F32)
    loads[1].wait()
    qrows = qh[...].astype(BF)
    qe[a] = dot(qrows, proj[...], ((1,), (0,))).astype(BF)
    loads[2].wait()
    pe[b] = dot(ph[...], proj[...], ((1,), (0,))).astype(BF)
    pl.semaphore_wait(barrier, PB + PA - 2)

    query_in = []
    for o in range(1, PA):
        c = remote(qe.at[a], qe.at[a], qs.at[o - 1], qr.at[o - 1], b, lax.rem(a + o, PA))
        c.start()
        query_in.append(c)
    page_in = {}
    for k in range(PB - 1, 0, -1):
        c = remote(pe.at[b], pe.at[b], ps.at[k - 1], pr.at[k - 1], group(k), a)
        c.start()
        page_in[k] = c

    step = min(256, hidden)
    for s in range(0, hidden, step):
        pht[s:s + step] = ph[:, s:s + step].T

    for c in query_in:
        c.wait_recv()
    tok = qe[...].reshape(tokens, E)
    row = lax.broadcasted_iota(jnp.int32, (queries, tokens), 0) * token_local
    col = lax.broadcasted_iota(jnp.int32, (queries, tokens), 1)
    mask = jnp.zeros((queries, tokens), F32)
    for k in range(PA):
        low = row + k * rows
        mask = jnp.where((col >= low) & (col < low + token_local), 1.0, mask)
    maxes, sums = [], []
    for k in range(PB):
        if k:
            page_in[k].wait_recv()
        block = sharpness * dot(pe[source(k)], tok, ((1,), (1,)))
        top = jnp.max(block, axis=0, keepdims=True)
        e = jnp.exp(block - top)
        ebuf[k] = e
        maxes.append(top)
        sums.append(jnp.sum(e, axis=0, keepdims=True))
    top = functools.reduce(jnp.maximum, maxes)
    shrink = [jnp.exp(m - top) for m in maxes]
    total = functools.reduce(jnp.add, [s * f for s, f in zip(sums, shrink)])
    log_norm = top + jnp.log(total)
    score = jnp.sum(mask * log_norm, axis=1, keepdims=True)
    sc[a] = jnp.broadcast_to(score, sc.shape[1:])
    score_in = []
    for o in range(1, PA):
        c = remote(sc.at[a], sc.at[a], ss.at[o - 1], sr.at[o - 1], b, lax.rem(a + o, PA))
        c.start()
        score_in.append(c)

    unit = None
    for k in range(PB):
        soft = (ebuf[k] * (shrink[k] / total)).astype(BF)
        pbuf[k] = soft
        part = dot(soft, pe[source(k)], ((0,), (0,)))
        unit = part if unit is None else unit + part
    for k in range(PA):
        tsend[k] = unit[k * rows:(k + 1) * rows].astype(BF)
    token_in = []
    for o in range(1, PA):
        to = lax.rem(a + o, PA)
        c = remote(tsend.at[to], trecv.at[a], ts.at[o - 1], tr.at[o - 1], b, to)
        c.start()
        token_in.append(c)
    trecv[a] = tsend[a]

    loads[3].wait()
    loads[4].wait()
    pos = clicks_ref[:, 0, :]
    neg = clicks_ref[:, 1, :]
    pairs = pos.shape[1]
    weight = jnp.sqrt(bins_ref[...].astype(F32) + 1.0)
    for c in score_in:
        c.wait_recv()
    at_pos = jnp.zeros(pos.shape, F32)
    at_neg = jnp.zeros(pos.shape, F32)
    for p in range(PA):
        at_pos = at_pos + jnp.where(pos == p, sc[p][:, :pairs], 0.0)
        at_neg = at_neg + jnp.where(neg == p, sc[p][:, :pairs], 0.0)
    coeff = -weight * jax.nn.sigmoid(at_neg - at_pos)
    row = lax.broadcasted_iota(jnp.int32, (rows, queries), 0)
    col = lax.broadcasted_iota(jnp.int32, (rows, queries), 1) * token_local
    own = jnp.where((row >= col) & (row < col + token_local), 1.0, 0.0)

    def spread(page):
        hits = (pos == page).astype(F32) - (neg == page).astype(F32)
        grad = jnp.sum(coeff * hits, axis=1, keepdims=True)
        return sum(own[:, q:q + 1] * grad[q:q + 1] for q in range(queries))

    scaled = (qe[...].astype(F32) * spread(a)[None]).astype(BF).reshape(tokens, E)
    patch_in = []
    for k in range(PB - 1, -1, -1):
        patch_part = dot(pbuf[k], scaled, ((1,), (0,)))
        if k:
            gsend[k - 1] = patch_part.astype(BF)
            c = remote(
                gsend.at[k - 1], grecv.at[k - 1], gs.at[k - 1], gr.at[k - 1],
                source(k), a,
            )
            c.start()
            patch_in.append((k, c))
        else:
            patch_acc = patch_part

    for c in token_in:
        c.wait_recv()
    token_own = None
    for p in range(PA):
        part = trecv[p].astype(F32) * spread(p)
        token_own = part if token_own is None else token_own + part
    token_low = (sharpness * token_own).astype(BF)
    wq[...] = dot(qrows, token_low, ((0,), (0,)))
    qgrad = dot(token_low, proj[...], ((1,), (1,)))
    for q in range(queries):
        qg_ref[q] = qgrad[q * token_local:(q + 1) * token_local].astype(BF)

    for k, c in reversed(patch_in):
        c.wait_recv()
        patch_acc = patch_acc + grecv[k - 1].astype(F32)
    patch_low = (sharpness * patch_acc).astype(BF)

    partner = b + 1 - 2 * parity
    span = w1send.shape[1]
    chunk = w_ref.shape[0]
    def weight_block(index):
        base = pl.multiple_of(index * span, 8)
        return wq[pl.ds(base, span)] + dot(pht[pl.ds(base, span)], patch_low, ((1,), (0,)))

    pair_in = {}
    for m in range(half - 1, -1, -1):
        w1send[m] = weight_block(2 * lax.rem(level + m, half) + 1 - parity).astype(BF)
        c = remote(w1send.at[m], w1recv.at[m], us.at[m], ur.at[m], partner, a)
        c.start()
        pair_in[m] = c
    last_in = []
    weight_own = None
    for m in range(half - 1, -1, -1):
        to_level = lax.rem(level + m, half)
        mine = weight_block(2 * to_level + parity)
        pair_in[m].wait_recv()
        both = (mine + w1recv[m].astype(F32)).astype(BF)
        for k in range(PA):
            w2send[m * PA + k] = both[k * chunk:(k + 1) * chunk]
        for o in range(PA - 1, -1, -1):
            slot = m * PA + o
            if slot:
                to = lax.rem(a + o, PA)
                c = remote(
                    w2send.at[m * PA + to], w2recv.at[slot - 1], vs.at[slot - 1],
                    vr.at[slot - 1], 2 * to_level + parity, to,
                )
                c.start()
                last_in.append((slot, c))
    pg_ref[...] = dot(patch_low, proj[...], ((1,), (1,))).astype(BF)
    weight_sum = w2send[a].astype(F32)
    for slot, c in last_in:
        c.wait_recv()
        weight_sum = weight_sum + w2recv[slot - 1].astype(F32)
    w_ref[...] = weight_sum
    last_in = [c for _, c in last_in]
    pair_in = list(pair_in.values())
    for c in list(page_in.values()) + query_in + score_in + [c for _, c in patch_in] + token_in + pair_in + last_in:
        c.wait_send()


def writer(qg, pg, w, qg_out, pg_out, w_out, sems):
    copies = [
        pltpu.make_async_copy(pg, pg_out, sems.at[0]),
        pltpu.make_async_copy(qg, qg_out, sems.at[1]),
        pltpu.make_async_copy(w, w_out, sems.at[2]),
    ]
    for c in copies:
        c.start()
    for c in copies:
        c.wait()


def shards(PB, PA, query_hidden, page_hidden, projection, clicks, bins):
    queries, token_local, hidden = query_hidden.shape
    page_count, patches, _ = page_hidden.shape
    assert page_count == 1 and PB % 2 == 0
    E = projection.shape[1]
    rows = queries * token_local
    tokens = rows * PA
    chunk = hidden // (PB * PA)
    half = PB // 2
    count = half * PA
    ph = page_hidden.reshape(patches, hidden)
    vmem = pl.BlockSpec(memory_space=pltpu.VMEM)
    hbm = pl.BlockSpec(memory_space=pltpu.HBM)
    dma = lambda n: pltpu.SemaphoreType.DMA((n,))
    outs = (
        jax.ShapeDtypeStruct(query_hidden.shape, BF),
        jax.ShapeDtypeStruct((patches, hidden), BF),
        jax.ShapeDtypeStruct((chunk, E), F32),
    )
    results = pl.pallas_call(
        functools.partial(kernel, PB, PA),
        out_shape=tuple(pltpu.VMEM(o.shape, o.dtype) for o in outs),
        in_specs=[hbm] * 5,
        out_specs=(vmem,) * 3,
        scratch_shapes=[
            pltpu.VMEM((queries, 2, clicks.shape[1]), jnp.int32),
            pltpu.VMEM(bins.shape, jnp.int32),
            pltpu.VMEM(query_hidden.shape, BF),
            pltpu.VMEM((rows, hidden), F32),
            pltpu.VMEM((patches, hidden), BF),
            pltpu.VMEM((hidden, patches), BF),
            pltpu.VMEM((hidden, E), BF),
            pltpu.VMEM((PA, rows, E), BF),
            pltpu.VMEM((PB, patches, E), BF),
            pltpu.VMEM((PB, patches, tokens), F32),
            pltpu.VMEM((PB, patches, tokens), BF),
            pltpu.VMEM((PA, queries, 128), F32),
            pltpu.VMEM((PB - 1, patches, E), BF),
            pltpu.VMEM((PB - 1, patches, E), BF),
            pltpu.VMEM((PA, rows, E), BF),
            pltpu.VMEM((PA, rows, E), BF),
            pltpu.VMEM((hidden, E), F32),
            pltpu.VMEM((half, PA * chunk, E), BF),
            pltpu.VMEM((half, PA * chunk, E), BF),
            pltpu.VMEM((count, chunk, E), BF),
            pltpu.VMEM((count - 1, chunk, E), BF),
            dma(5), dma(PA - 1), dma(PA - 1), dma(PB - 1), dma(PB - 1), dma(PA - 1), dma(PA - 1),
            dma(PB - 1), dma(PB - 1), dma(PA - 1), dma(PA - 1), dma(half), dma(half),
            dma(count - 1), dma(count - 1),
        ],
        compiler_params=pltpu.CompilerParams(
            collective_id=0, has_side_effects=True, vmem_limit_bytes=65536000
        ),
        name="fused",
    )(query_hidden, ph, projection, jnp.transpose(clicks, (0, 2, 1)), bins)
    query_grad, page_grad, weight_grad = pl.pallas_call(
        writer,
        out_shape=outs,
        in_specs=[vmem] * 3,
        out_specs=(hbm,) * 3,
        scratch_shapes=[dma(3)],
        compiler_params=pltpu.CompilerParams(vmem_limit_bytes=4 * 1024 * 1024),
        name="writer",
    )(*results)
    return query_grad, page_grad.reshape(page_hidden.shape), weight_grad


def solution(mesh):
    return jax.shard_map(
        functools.partial(shards, mesh.shape["pb"], mesh.shape["pa"]),
        mesh=mesh,
        in_specs=(
            P("pb", "pa", None),
            P("pa", "pb", None),
            P(),
            P("pb", None, None),
            P("pb", None),
        ),
        out_specs=(P("pb", "pa", None), P("pa", "pb", None), P(("pb", "pa"), None)),
        check_vma=False,
    )
```
